32 devices in a mesh: dp: 4 (over y, core), tensor: 8 (over z, x).
Axes of the slice: x: 2, y: 2, z: 4, core: 2. Of those that a mesh axis runs over, the one named last changes fastest.
Arguments:
- query_latent: bfloat16 [64, 1536], P(('dp', 'tensor')), may hold values from -40 to 40
- key_value_latent: bfloat16 [64, 512], P(('dp', 'tensor')), may hold values from -40 to 40
- query_gain: float32 [1536], replicated, may hold values from 0.5 to 1.5
- key_value_gain: float32 [512], replicated, may hold values from 0.5 to 1.5
- q_up: bfloat16 [1536, 3072], P(None, 'tensor'), may hold values from -0.625 to 0.625
- kv_up: bfloat16 [512, 4096], P(None, 'tensor'), may hold values from -1 to 1
- grad_q: bfloat16 [64, 3072], P('dp', 'tensor'), may hold values from -0.23925781 to 0.23925781
- grad_kv: bfloat16 [64, 4096], P('dp', 'tensor'), may hold values from -0.23925781 to 0.23925781
Outputs:
- query_latent_gradient: float32 [64, 1536], P(('dp', 'tensor'))
- key_value_latent_gradient: float32 [64, 512], P(('dp', 'tensor'))
- d_q_up: float32 [1536, 3072], P('dp', 'tensor')
- d_kv_up: float32 [512, 4096], P('dp', 'tensor')
The draws below stay inside these ranges and needn't reach their ends.
All inputs are finite; a program needn't handle non-finite values.
Results may differ from the reference program's by a relative error of at most 0.0029.
Values may be sent and summed in bfloat16 or wider, within the bound.
No kernel may reach another device: no remote copies, remote signals or barrier semaphores. Data moves between devices by JAX's collectives and lax.ppermute only.
A program may use at most 64 MiB of HBM per device.

```python
import math
import jax
import jax.numpy as jnp
from jax import lax

QL = 1536
KVL = 512
NOPE = 128
ROPE = 64
VDIM = 128
HEADS = 16
TOK_ALL = 64
N_DP = 4


def scaled_latent(key, rows, cols):
    key_rows, key_cols, key_base = jax.random.split(key, 3)
    row_scale = 0.3 * jnp.exp(jax.random.uniform(key_rows, (rows, 1), minval=0.0, maxval=math.log(10.0)))
    col_scale = 0.3 * jnp.exp(jax.random.uniform(key_cols, (1, cols), minval=0.0, maxval=math.log(10.0)))
    base = jax.random.normal(key_base, (rows, cols))
    input_values = jnp.clip(base * row_scale * col_scale, -40.0, 40.0)
    return input_values.astype(jnp.bfloat16)


def draw_query_latent(key, part):
    return scaled_latent(jax.random.fold_in(key, 11), TOK_ALL, QL)


def draw_key_value_latent(key, part):
    return scaled_latent(jax.random.fold_in(key, 23), TOK_ALL, KVL)


def steps_of(own_key, extent, cuts, low, high):
    def one(dim, shards_of):
        heights = jax.random.uniform(jax.random.fold_in(jax.random.fold_in(own_key, 6), dim), (shards_of,), jnp.float32, low / len(cuts), high / len(cuts))
        return jnp.repeat(jnp.exp(heights), extent[dim] // shards_of).reshape((-1,) + (1,) * (len(extent) - dim - 1))

    factor_of = one(*cuts[0])
    for cut in cuts[1:]:
        factor_of = factor_of * one(*cut)
    return factor_of


def centred(key, shape, scale, bound, cuts=(), held_as=jnp.bfloat16):
    drawn = jax.random.normal(key, shape, jnp.float32) * scale
    if len(cuts) > 0:
        drawn = steps_of(key, shape, cuts, -0.22, 0.18) * drawn
    return jnp.clip(drawn, min=-bound, max=bound).astype(held_as)


def setup_inputs(seed: int = 0) -> dict:
    streams_of = jax.random.split(jax.random.key(seed), 9)
    query_latent = draw_query_latent(jax.random.fold_in(streams_of[8], 71), 0)
    key_value_latent = draw_key_value_latent(jax.random.fold_in(streams_of[8], 71), 0)
    query_gain = jnp.clip(1.0 + 0.1 * jax.random.normal(streams_of[2], (QL,), jnp.float32), 0.5, 1.5)
    key_value_gain = jnp.clip(1.0 + 0.1 * jax.random.normal(streams_of[3], (KVL,), jnp.float32), 0.5, 1.5)
    q_up = centred(streams_of[4], (QL, HEADS * (NOPE + ROPE)), (QL // 16) ** -0.5, 0.625, ((1, 8),))
    kv_up = centred(streams_of[5], (KVL, HEADS * (NOPE + VDIM)), (KVL // 16) ** -0.5, 1.0, ((1, 8),))
    grad_q = centred(streams_of[6], (TOK_ALL, HEADS * (NOPE + ROPE)), 0.04, 0.23925781, ((0, 4), (1, 8)))
    grad_kv = centred(streams_of[7], (TOK_ALL, HEADS * (NOPE + VDIM)), 0.04, 0.23925781, ((0, 4), (1, 8)))
    return {"query_latent": query_latent, "key_value_latent": key_value_latent, "query_gain": query_gain, "key_value_gain": key_value_gain, "q_up": q_up, "kv_up": kv_up, "grad_q": grad_q, "grad_kv": grad_kv}


EPS = 1e-06

def apply_norm(raw, norm_gain):
    input_values = raw.astype(jnp.float32)
    inverse_norm = lax.rsqrt(lax.optimization_barrier(jnp.mean(input_values * input_values, axis=-1, keepdims=True)) + EPS)
    unit_input = input_values * inverse_norm
    return (unit_input, inverse_norm, (norm_gain * unit_input).astype(jnp.bfloat16))

def backward_of_norm(incoming_gradient, unit_input, inverse_norm, norm_gain):
    scaled_gradient = norm_gain * incoming_gradient
    mean_correction = lax.optimization_barrier(jnp.mean(scaled_gradient * unit_input, axis=-1, keepdims=True))
    return inverse_norm * (scaled_gradient - unit_input * mean_correction)

def group_weights(normed, cotangent):
    groups = normed.reshape(N_DP, -1, normed.shape[1])
    cot_groups = cotangent.reshape(N_DP, -1, cotangent.shape[1])

    def step(total, pair):
        part = lax.dot_general(pair[0], pair[1], (((0,), (0,)), ((), ())), preferred_element_type=jnp.float32)
        return (total + part, None)
    start = jnp.zeros((normed.shape[1], cotangent.shape[1]), jnp.float32)
    total, unused_item = lax.scan(step, start, (groups, cot_groups))
    return total

def reference(query_latent, key_value_latent, query_gain, key_value_gain, q_up, kv_up, grad_q, grad_kv):
    query_unit, query_inverse_norm, query_normed = apply_norm(query_latent, query_gain)
    key_value_unit, key_value_inverse_norm, key_value_normed = apply_norm(key_value_latent, key_value_gain)
    d_q_up = group_weights(query_normed, grad_q)
    d_kv_up = group_weights(key_value_normed, grad_kv)
    query_norm_gain = lax.dot_general(grad_q, q_up, (((1,), (1,)), ((), ())), preferred_element_type=jnp.float32)
    key_value_norm_gain = lax.dot_general(grad_kv, kv_up, (((1,), (1,)), ((), ())), preferred_element_type=jnp.float32)
    query_latent_gradient = backward_of_norm(query_norm_gain, query_unit, query_inverse_norm, query_gain)
    key_value_latent_gradient = backward_of_norm(key_value_norm_gain, key_value_unit, key_value_inverse_norm, key_value_gain)
    return (query_latent_gradient, key_value_latent_gradient, d_q_up, d_kv_up)
```

```python
import jax
import jax.numpy as jnp
from jax import lax
from jax.sharding import PartitionSpec as P

EPS = 1e-06


def apply_norm(raw, norm_gain):
    input_values = raw.astype(jnp.float32)
    inverse_norm = lax.rsqrt(jnp.mean(input_values * input_values, axis=-1, keepdims=True) + EPS)
    unit_input = input_values * inverse_norm
    return (unit_input, inverse_norm, (norm_gain * unit_input).astype(jnp.bfloat16))


def backward_of_norm(incoming_gradient, unit_input, inverse_norm, norm_gain):
    scaled_gradient = norm_gain * incoming_gradient
    mean_correction = jnp.mean(scaled_gradient * unit_input, axis=-1, keepdims=True)
    return inverse_norm * (scaled_gradient - unit_input * mean_correction)


def contract_rows(left, right):
    return lax.dot_general(
        left, right, (((0,), (0,)), ((), ())), preferred_element_type=jnp.float32
    )


def contract_cols(left, right):
    return lax.dot_general(
        left, right, (((1,), (1,)), ((), ())), preferred_element_type=jnp.float32
    )


def dp_pairs(size, step):
    if size & (size - 1) == 0:
        return [(i, i ^ step) for i in range(size)]
    return [(i, (i + step) % size) for i in range(size)]


def body(n_dp, n_tensor, query_latent, key_value_latent, query_gain, key_value_gain, q_up, kv_up, grad_q, grad_kv):
    own, q_width = query_latent.shape
    kv_width = key_value_latent.shape[1]
    tokens, q_cols = grad_q.shape
    q_rows, kv_rows = q_width // n_dp, kv_width // n_dp
    rows = q_rows + kv_rows
    me = lax.axis_index("dp")

    q_unit, q_inverse, q_normed = apply_norm(query_latent, query_gain)
    kv_unit, kv_inverse, kv_normed = apply_norm(key_value_latent, key_value_gain)
    slices = jnp.concatenate(
        (q_normed.reshape(own, n_dp, q_rows), kv_normed.reshape(own, n_dp, kv_rows)), axis=2
    ).transpose(1, 0, 2)
    grads = jnp.concatenate((grad_q, grad_kv), axis=1)

    latents, all_grads = [lax.dynamic_index_in_dim(slices, me, 0, keepdims=False)], [grads]
    for step in range(1, n_dp):
        pairs = dp_pairs(n_dp, step)
        target = jnp.asarray([t for _, t in pairs], jnp.int32)[me]
        sent = lax.dynamic_index_in_dim(slices, target, 0, keepdims=False)
        packed = jnp.concatenate((grads, sent.reshape(tokens, -1)), axis=1)
        came = lax.ppermute(packed, "dp", pairs)
        all_grads.append(came[:, : grads.shape[1]])
        latents.append(came[:, grads.shape[1] :].reshape(own, rows))

    part = jnp.concatenate((contract_cols(grad_q, q_up), contract_cols(grad_kv, kv_up)), axis=1)
    part = part.reshape(n_tensor, own, q_width + kv_width)
    high = part.astype(jnp.bfloat16)
    low = (part - high.astype(jnp.float32)).astype(jnp.bfloat16)
    latent = jnp.concatenate(latents, axis=1)
    message = jnp.concatenate(
        (high, low, jnp.broadcast_to(latent[None], (n_tensor,) + latent.shape)), axis=2
    )
    came = lax.all_to_all(message, "tensor", 0, 0)
    width = q_width + kv_width
    summed = jnp.sum(
        came[:, :, :width].astype(jnp.float32) + came[:, :, width : 2 * width].astype(jnp.float32), axis=0
    )
    normed = [
        came[:, :, 2 * width + s * rows : 2 * width + (s + 1) * rows].reshape(tokens, rows)
        for s in range(n_dp)
    ]
    normed = jnp.concatenate(normed, axis=0)
    all_grads = jnp.concatenate(all_grads, axis=0)
    return (
        backward_of_norm(summed[:, :q_width], q_unit, q_inverse, query_gain),
        backward_of_norm(summed[:, q_width:], kv_unit, kv_inverse, key_value_gain),
        contract_rows(normed[:, :q_rows], all_grads[:, :q_cols]),
        contract_rows(normed[:, q_rows:], all_grads[:, q_cols:]),
    )


def solution(mesh):
    n_dp, n_tensor = mesh.shape["dp"], mesh.shape["tensor"]
    return jax.shard_map(
        lambda *args: body(n_dp, n_tensor, *args),
        mesh=mesh,
        in_specs=(
            P(("dp", "tensor"), None),
            P(("dp", "tensor"), None),
            P(),
            P(),
            P(None, "tensor"),
            P(None, "tensor"),
            P("dp", "tensor"),
            P("dp", "tensor"),
        ),
        out_specs=(
            P(("dp", "tensor"), None),
            P(("dp", "tensor"), None),
            P("dp", "tensor"),
            P("dp", "tensor"),
        ),
        check_vma=False,
    )
```

```python
import functools

import jax
import jax.numpy as jnp
from jax import lax
from jax.experimental import pallas as pl
from jax.experimental.pallas import tpu as pltpu
from jax.sharding import PartitionSpec as P

EPS = 1e-06
CHUNKS = 3
VMEM = 16 * 1024 * 1024


def dp_pairs(size, step):
    if size & (size - 1) == 0:
        return [(i, i ^ step) for i in range(size)]
    return [(i, (i + step) % size) for i in range(size)]


def dp_source(size, step, me):
    if size & (size - 1) == 0:
        return jnp.bitwise_xor(me, step)
    return lax.rem(me + size - step, size)


def unit_of(raw):
    values = raw.astype(jnp.float32)
    inverse = lax.rsqrt(jnp.mean(values * values, axis=-1, keepdims=True) + EPS)
    return values * inverse, inverse


def contract_cols(left, right):
    return lax.dot_general(
        left, right, (((1,), (1,)), ((), ())), preferred_element_type=jnp.float32
    )


def contract_rows(left, right):
    return lax.dot_general(
        left, right, (((0,), (0,)), ((), ())), preferred_element_type=jnp.float32
    )


def first_kernel(n_dp, n_tensor, chunks, *refs):
    sources, (part, latent, grads), rest = refs[:8], refs[8:11], refs[11:]
    held, sems = rest[:8], rest[8]
    q_lat, kv_lat, q_gain, kv_gain, q_up, kv_up, grad_q, grad_kv = held
    own, q_width = q_lat.shape
    kv_width = kv_lat.shape[1]
    q_cols = grad_q.shape[1]
    q_rows, kv_rows = q_width // n_dp, kv_width // n_dp
    step = q_width // chunks

    def fetch(i):
        return pltpu.make_async_copy(sources[i], held[i], sems.at[i])

    def fetch_rows(c):
        at = pl.ds(c * step, step)
        return pltpu.make_async_copy(sources[4].at[at], q_up.at[at], sems.at[8 + c])

    for i in (0, 1, 2, 3, 6, 7, 5):
        fetch(i).start()
    for c in range(chunks):
        fetch_rows(c).start()
    for i in (0, 1, 2, 3):
        fetch(i).wait()
    q_normed = (q_gain[...][None] * unit_of(q_lat[...])[0]).astype(jnp.bfloat16)
    kv_normed = (kv_gain[...][None] * unit_of(kv_lat[...])[0]).astype(jnp.bfloat16)
    for d in range(n_dp):
        piece = jnp.concatenate(
            (q_normed[:, d * q_rows : (d + 1) * q_rows], kv_normed[:, d * kv_rows : (d + 1) * kv_rows]), axis=1
        )
        latent[d * n_tensor : (d + 1) * n_tensor] = jnp.broadcast_to(piece[None], (n_tensor,) + piece.shape)
    for i in (6, 7):
        fetch(i).wait()
    grads[:, :q_cols] = grad_q[...]
    grads[:, q_cols:] = grad_kv[...]

    def put(value, at):
        for t in range(n_tensor):
            part[t, :, at : at + value.shape[1]] = value[t * own : (t + 1) * own]

    fetch(5).wait()
    put(contract_cols(grad_kv[...], kv_up[...]), q_width)
    for c in range(chunks):
        fetch_rows(c).wait()
        put(contract_cols(grad_q[...], q_up[c * step : (c + 1) * step]), c * step)


def latent_kernel(part, q_lat, kv_lat, q_gain, kv_gain, q_out, kv_out):
    q_width = q_lat.shape[1]
    summed = jnp.sum(part[...], axis=0)
    for out, raw, gain, incoming in (
        (q_out, q_lat, q_gain, summed[:, :q_width]),
        (kv_out, kv_lat, kv_gain, summed[:, q_width:]),
    ):
        unit, inverse = unit_of(raw[...])
        scaled = gain[...][None] * incoming
        out[...] = inverse * (scaled - unit * jnp.mean(scaled * unit, axis=-1, keepdims=True))


def weight_kernel(n_dp, latent, *refs):
    grads, (q_out, kv_out) = refs[:-2], refs[-2:]
    me = lax.axis_index("dp")
    tokens = grads[0].shape[0]
    q_rows, q_cols = q_out.shape
    order = []
    for step in range(n_dp):
        start = pl.multiple_of(dp_source(n_dp, step, me) * tokens, tokens)
        order.append(latent[pl.ds(start, tokens), :])
    normed = jnp.concatenate(order, axis=0)
    every = jnp.concatenate([g[...] for g in grads], axis=0)
    q_out[...] = contract_rows(normed[:, :q_rows], every[:, :q_cols])
    kv_out[...] = contract_rows(normed[:, q_rows:], every[:, q_cols:])


def struct(shape, dtype=jnp.float32):
    return jax.ShapeDtypeStruct(shape, dtype)


def cost(flops, nbytes):
    return pl.CostEstimate(flops=flops, bytes_accessed=nbytes, transcendentals=0)


def body(n_dp, n_tensor, q_lat, kv_lat, q_gain, kv_gain, q_up, kv_up, grad_q, grad_kv):
    own, q_width = q_lat.shape
    kv_width = kv_lat.shape[1]
    tokens, q_cols = grad_q.shape
    kv_cols = grad_kv.shape[1]
    q_rows, kv_rows = q_width // n_dp, kv_width // n_dp
    rows, width = q_rows + kv_rows, q_width + kv_width
    inputs = (q_lat, kv_lat, q_gain, kv_gain, q_up, kv_up, grad_q, grad_kv)
    part, latent, grads = pl.pallas_call(
        functools.partial(first_kernel, n_dp, n_tensor, CHUNKS),
        in_specs=[pl.BlockSpec(memory_space=pltpu.HBM)] * 8,
        scratch_shapes=[pltpu.VMEM(x.shape, x.dtype) for x in inputs]
        + [pltpu.SemaphoreType.DMA((8 + CHUNKS,))],
        out_shape=(
            struct((n_tensor, own, width)),
            struct((n_dp * n_tensor, own, rows), jnp.bfloat16),
            struct((tokens, q_cols + kv_cols), jnp.bfloat16),
        ),
        cost_estimate=cost(2 * tokens * (q_cols * q_width + kv_cols * kv_width), 4000000),
        compiler_params=pltpu.CompilerParams(vmem_limit_bytes=VMEM),
        name="first",
    )(*[pltpu.with_memory_space_constraint(x, pltpu.HBM) for x in inputs])
    part = lax.all_to_all(part, "tensor", 0, 0)
    latent = lax.all_to_all(latent, ("dp", "tensor"), 0, 0)
    all_grads = [grads] + [lax.ppermute(grads, "dp", dp_pairs(n_dp, s)) for s in range(1, n_dp)]
    q_out, kv_out = pl.pallas_call(
        latent_kernel,
        out_shape=(struct(q_lat.shape), struct(kv_lat.shape)),
        cost_estimate=cost(10000, 200000),
        compiler_params=pltpu.CompilerParams(vmem_limit_bytes=VMEM),
        name="latent",
    )(part, q_lat, kv_lat, q_gain, kv_gain)
    q_weight, kv_weight = pl.pallas_call(
        functools.partial(weight_kernel, n_dp),
        out_shape=(struct((q_rows, q_cols)), struct((kv_rows, kv_cols))),
        cost_estimate=cost(2 * n_dp * tokens * (q_rows * q_cols + kv_rows * kv_cols), 1000000),
        compiler_params=pltpu.CompilerParams(vmem_limit_bytes=VMEM),
        name="weight",
    )(latent.reshape(n_dp * tokens, rows), *all_grads)
    return q_out, kv_out, q_weight, kv_weight


def solution(mesh):
    n_dp, n_tensor = mesh.shape["dp"], mesh.shape["tensor"]
    return jax.shard_map(
        functools.partial(body, n_dp, n_tensor),
        mesh=mesh,
        in_specs=(
            P(("dp", "tensor"), None),
            P(("dp", "tensor"), None),
            P(),
            P(),
            P(None, "tensor"),
            P(None, "tensor"),
            P("dp", "tensor"),
            P("dp", "tensor"),
        ),
        out_specs=(
            P(("dp", "tensor"), None),
            P(("dp", "tensor"), None),
            P("dp", "tensor"),
            P("dp", "tensor"),
        ),
        check_vma=False,
    )
```

```python
import functools

import jax
import jax.numpy as jnp
from jax import lax
from jax.experimental import pallas as pl
from jax.experimental.pallas import tpu as pltpu
from jax.sharding import PartitionSpec as P

EPS = 1e-06
VMEM = 16 * 1024 * 1024


def dp_pairs(size, step):
    if size & (size - 1) == 0:
        return [(i, i ^ step) for i in range(size)]
    return [(i, (i + step) % size) for i in range(size)]


def order_of(size):
    return [(size - 1 - i) ^ 1 for i in range(size)]


def dp_target(size, step, me):
    if size & (size - 1) == 0:
        return jnp.bitwise_xor(me, step)
    return lax.rem(me + step, size)


def unit_of(raw):
    values = raw.astype(jnp.float32)
    inverse = lax.rsqrt(jnp.mean(values * values, axis=-1, keepdims=True) + EPS)
    return values * inverse, inverse


def contract_cols(left, right):
    return lax.dot_general(
        left, right, (((1,), (1,)), ((), ())), preferred_element_type=jnp.float32
    )


def contract_rows(left, right):
    return lax.dot_general(
        left, right, (((0,), (0,)), ((), ())), preferred_element_type=jnp.float32
    )


def fetched(kernel, inputs, outputs, *refs):
    sources, outs, scratch = refs[:inputs], refs[inputs : inputs + outputs], refs[inputs + outputs :]
    held, sems = scratch[:inputs], scratch[inputs]
    copies = [pltpu.make_async_copy(a, b, sems.at[i]) for i, (a, b) in enumerate(zip(sources, held))]
    for copy in copies:
        copy.start()
    kernel([copy.wait for copy in copies], *held, *outs, *scratch[inputs + 1 :])


def norm_kernel(n_dp, waits, q_lat, kv_lat, q_gain, kv_gain, grad_q, grad_kv, *outs):
    slices, messages = outs[-1], outs[:-1]
    for wait in waits:
        wait()
    own, q_width = q_lat.shape
    kv_width = kv_lat.shape[1]
    tokens, q_cols = grad_q.shape
    cols = q_cols + grad_kv.shape[1]
    q_rows, kv_rows = q_width // n_dp, kv_width // n_dp
    q_normed = (q_gain[...][None] * unit_of(q_lat[...])[0]).astype(jnp.bfloat16)
    kv_normed = (kv_gain[...][None] * unit_of(kv_lat[...])[0]).astype(jnp.bfloat16)
    for d in range(n_dp):
        slices[d] = jnp.concatenate(
            (q_normed[:, d * q_rows : (d + 1) * q_rows], kv_normed[:, d * kv_rows : (d + 1) * kv_rows]), axis=1
        )
    me = lax.axis_index("dp")
    for step, message in enumerate(messages):
        piece = slices[dp_target(n_dp, step, me)]
        message[:tokens, :q_cols] = grad_q[...]
        message[:tokens, q_cols:cols] = grad_kv[...]
        width = message.shape[1] - cols
        for i in range((q_rows + kv_rows) // width):
            message[i * own : (i + 1) * own, cols:] = piece[:, i * width : (i + 1) * width]


def part_kernel(order, waits, grad_q, grad_kv, kv_up, q_up, out):
    own = out.shape[1]
    q_width, kv_width = q_up.shape[0], kv_up.shape[0]
    width = q_width + kv_width
    waits[0]()
    waits[1]()
    for at, grad, up, wait in ((q_width, grad_kv, kv_up, waits[2]), (0, grad_q, q_up, waits[3])):
        wait()
        value = contract_cols(grad[...], up[...])
        size = value.shape[1]
        high = value.astype(jnp.bfloat16)
        low = (value - high.astype(jnp.float32)).astype(jnp.bfloat16)
        for to, t in enumerate(order):
            rows = slice(t * own, (t + 1) * own)
            out[to, :, at : at + size] = high[rows]
            out[to, :, width + at : width + at + size] = low[rows]


def pack_kernel(n_dp, cols, start, rows, *refs):
    messages, out = refs[:n_dp], refs[-1]
    n_tensor, own = out.shape[:2]
    width = messages[0].shape[1] - cols
    for s, message in enumerate(messages):
        for i in range(rows // width):
            piece = message[i * own : (i + 1) * own, cols:]
            at = start + s * rows + i * width
            out[:, :, at : at + width] = jnp.broadcast_to(piece[None], (n_tensor,) + piece.shape)


def final_kernel(n_dp, cols, order, q_lat, kv_lat, q_gain, kv_gain, came, *refs):
    messages, (q_out, kv_out, q_weight, kv_weight) = refs[:n_dp], refs[n_dp:]
    n_tensor, own, _ = came.shape
    q_width, kv_width = q_lat.shape[1], kv_lat.shape[1]
    width = q_width + kv_width
    q_rows, q_cols = q_weight.shape
    rows = q_rows + kv_weight.shape[0]
    tokens = n_tensor * own
    normed, grads = [], []
    for s in range(n_dp):
        at = 2 * width + s * rows
        normed += [came[order.index(t), :, at : at + rows] for t in range(n_tensor)]
        grads.append(messages[s][:tokens, :cols])
    normed = jnp.concatenate(normed, axis=0)
    grads = jnp.concatenate(grads, axis=0)
    q_weight[...] = contract_rows(normed[:, :q_rows], grads[:, :q_cols])
    kv_weight[...] = contract_rows(normed[:, q_rows:], grads[:, q_cols:])
    summed = jnp.sum(
        came[:, :, :width].astype(jnp.float32) + came[:, :, width : 2 * width].astype(jnp.float32), axis=0
    )
    for out, raw, gain, incoming in (
        (q_out, q_lat, q_gain, summed[:, :q_width]),
        (kv_out, kv_lat, kv_gain, summed[:, q_width:]),
    ):
        unit, inverse = unit_of(raw[...])
        scaled = gain[...][None] * incoming
        out[...] = inverse * (scaled - unit * jnp.mean(scaled * unit, axis=-1, keepdims=True))


def call_fetched(kernel, name, flops, out_shape, inputs, scratch_shapes=()):
    outs = len(out_shape) if isinstance(out_shape, (list, tuple)) else 1
    return call(
        functools.partial(fetched, kernel, len(inputs), outs),
        name,
        flops,
        out_shape,
        in_specs=[pl.BlockSpec(memory_space=pltpu.HBM)] * len(inputs),
        scratch_shapes=[pltpu.VMEM(x.shape, x.dtype) for x in inputs]
        + [pltpu.SemaphoreType.DMA((len(inputs),))]
        + list(scratch_shapes),
    )(*[pltpu.with_memory_space_constraint(x, pltpu.HBM) for x in inputs])


def call(kernel, name, flops, out_shape, **kwargs):
    return pl.pallas_call(
        kernel,
        out_shape=out_shape,
        cost_estimate=pl.CostEstimate(flops=flops, bytes_accessed=1000000, transcendentals=0),
        compiler_params=pltpu.CompilerParams(vmem_limit_bytes=VMEM),
        name=name,
        **kwargs,
    )


def struct(shape, dtype=jnp.float32):
    return jax.ShapeDtypeStruct(shape, dtype)


def body(n_dp, n_tensor, q_lat, kv_lat, q_gain, kv_gain, q_up, kv_up, grad_q, grad_kv):
    own, q_width = q_lat.shape
    kv_width = kv_lat.shape[1]
    tokens, q_cols = grad_q.shape
    kv_cols = grad_kv.shape[1]
    q_rows, kv_rows = q_width // n_dp, kv_width // n_dp
    rows, width, cols = q_rows + kv_rows, q_width + kv_width, q_cols + kv_cols
    extra = min(128, rows)
    messages = call_fetched(
        functools.partial(norm_kernel, n_dp),
        "norm",
        1000000,
        [struct((tokens, cols + extra), jnp.bfloat16)] * n_dp,
        (q_lat, kv_lat, q_gain, kv_gain, grad_q, grad_kv),
        [pltpu.VMEM((n_dp, own, rows), jnp.bfloat16)],
    )
    messages = [messages[0]] + [
        lax.ppermute(messages[s], "dp", dp_pairs(n_dp, s)) for s in range(1, n_dp)
    ]
    shape = struct((n_tensor, own, 2 * width + n_dp * rows), jnp.bfloat16)
    order = order_of(n_tensor)
    packed = call_fetched(
        functools.partial(part_kernel, order),
        "part",
        2 * tokens * (q_cols * q_width + kv_cols * kv_width),
        shape,
        (grad_q, grad_kv, kv_up, q_up),
    )
    packed = call(
        functools.partial(pack_kernel, n_dp, cols, 2 * width, rows),
        "pack",
        100000,
        shape,
        input_output_aliases={n_dp: 0},
    )(*messages, packed)
    came = lax.all_to_all(packed, "tensor", 0, 0, axis_index_groups=[order])
    return call(
        functools.partial(final_kernel, n_dp, cols, order),
        "final",
        2 * n_dp * tokens * (q_rows * q_cols + kv_rows * kv_cols),
        (
            struct(q_lat.shape),
            struct(kv_lat.shape),
            struct((q_rows, q_cols)),
            struct((kv_rows, kv_cols)),
        ),
    )(q_lat, kv_lat, q_gain, kv_gain, came, *messages)


def solution(mesh):
    n_dp, n_tensor = mesh.shape["dp"], mesh.shape["tensor"]
    return jax.shard_map(
        functools.partial(body, n_dp, n_tensor),
        mesh=mesh,
        in_specs=(
            P(("dp", "tensor"), None),
            P(("dp", "tensor"), None),
            P(),
            P(),
            P(None, "tensor"),
            P(None, "tensor"),
            P("dp", "tensor"),
            P("dp", "tensor"),
        ),
        out_specs=(
            P(("dp", "tensor"), None),
            P(("dp", "tensor"), None),
            P("dp", "tensor"),
            P("dp", "tensor"),
        ),
        check_vma=False,
    )
```
